128 devices in a mesh: layer: 8 (over x, z_hi), feat: 16 (over y, z_lo, core).
Axes of the slice: x: 4, y: 4, z: 4 (z_hi: 2, z_lo: 2; z = z_hi * 2 + z_lo), core: 2. Of those that a mesh axis runs over, the one named last changes fastest.
Arguments:
- residuals: bfloat16 [512, 4096], P('feat', 'layer'), may hold values from -6 to 6
- errors: bfloat16 [512, 4096], P('feat', 'layer'), may hold values from -0.26367188 to 0.26367188
- enc_weight: bfloat16 [4096, 65536], P('layer', 'feat'), may hold values from -0.09375 to 0.09375
- dec_weight: bfloat16 [4096, 65536], P('layer', 'feat'), may hold values from -0.09375 to 0.09375
- enc_bias: float32 [65536], P('feat'), may hold values from -3 to 3
Outputs:
- enc_grad: bfloat16 [4096, 65536], P('layer', 'feat')
- dec_grad: bfloat16 [4096, 65536], P('layer', 'feat')
- bias_grad: float32 [65536], P('feat')
The draws below stay inside these ranges and needn't reach their ends.
All inputs are finite; a program needn't handle non-finite values.
Results may differ from the reference program's by a relative error of at most 0.0055.
Values may be sent and summed in bfloat16 or wider, within the bound.
A program may use at most 128 MiB of HBM per device.

```python
import jax
import jax.numpy as jnp

FEATS = 65536
TOKENS = 512
STACK = 4096


def steps_of(rng, extent, cuts, least, high):
    def one(dim, blocks):
        heights = jax.random.uniform(jax.random.fold_in(jax.random.fold_in(rng, 6), dim), (blocks,), jnp.float32, least / len(cuts), high / len(cuts))
        return jnp.repeat(jnp.exp(heights), extent[dim] // blocks).reshape((-1,) + (1,) * (len(extent) - dim - 1))

    loudness = one(*cuts[0])
    for cut in cuts[1:]:
        loudness = loudness * one(*cut)
    return loudness


def gaussian(stream_key, shape, spread, reach, split=(), held_as=jnp.bfloat16):
    level = steps_of(stream_key, shape, split, -0.22, 0.18) if split else 1.0
    array = jax.random.normal(stream_key, shape, jnp.float32) * spread * level
    return jnp.minimum(jnp.maximum(array, -reach), reach).astype(held_as)


def setup_inputs(seed: int = 0) -> dict:
    seeds = jax.random.split(jax.random.key(seed), 6)
    return {
        "residuals": gaussian(seeds[0], (TOKENS, STACK), 1.0, 6.0, ((0, 16), (1, 8))),
        "errors": gaussian(seeds[1], (TOKENS, STACK), (TOKENS ** -0.5), 0.26367188, ((0, 16), (1, 8))),
        "enc_weight": gaussian(seeds[2], (STACK, FEATS), STACK ** -0.5, 0.09375, ((0, 8), (1, 16))),
        "dec_weight": gaussian(seeds[3], (STACK, FEATS), STACK ** -0.5, 0.09375, ((0, 8), (1, 16))),
        "enc_bias": gaussian(seeds[4], (FEATS,), 0.5, 3.0, ((0, 16),), jnp.float32),
    }


def reference(residuals, errors, enc_weight, dec_weight, enc_bias):
    preact = jnp.dot(residuals, enc_weight, preferred_element_type=jnp.float32) + enc_bias
    code_grad = jnp.dot(errors, dec_weight, preferred_element_type=jnp.float32)
    code = (jax.nn.softplus(4.0 * preact) / 4.0).astype(jnp.bfloat16)
    masked = (code_grad * jax.nn.sigmoid(4.0 * preact)).astype(jnp.bfloat16)
    enc_grad = jnp.dot(residuals.T, masked, preferred_element_type=jnp.float32).astype(jnp.bfloat16)
    dec_grad = jnp.dot(errors.T, code, preferred_element_type=jnp.float32).astype(jnp.bfloat16)
    bias_grad = jnp.sum(masked.astype(jnp.float32), axis=0)
    return enc_grad, dec_grad, bias_grad
```

```python
import functools

import jax
import jax.numpy as jnp
from jax import lax
from jax.experimental import pallas as pl
from jax.experimental.pallas import tpu as pltpu
from jax.sharding import PartitionSpec as P

MESH = pl.DeviceIdType.MESH
BF16, F32 = jnp.bfloat16, jnp.float32
CHUNKS = 8
ROWS = 64
HALF = ROWS // 2
STACKED = 512
WIDE, NARROW = 256, 128
SLOTS = ((2, 0), (1, 1), (2, 1), (3, 0), (1, 0), (3, 1), (0, 0), (0, 1))

KINDS = (
    "x1r", "x1l", "x2r", "x2l", "xz", "xgz", "xgr0", "xgl0", "xgr1", "xgl1", "xfr", "xfl",
    "z1", "z1r", "z1l", "z2r", "z2l", "zgr", "zgl", "zfr", "zfl", "zz0", "zz1", "zz3", "zz2",
)


def comm_kernel(
    resid, errors, enc, dec, bias,
    out_resid, out_errors, out_masked, out_code,
    re, xw, zw, xb, zb,
    xp, xr1, xr2, xzr, xo,
    zp, zr1, yr1, yr2, zo,
    send_sem, recv_sem, re_send, re_recv, own_sem, w_sem, out_sem, bias_sem, rout_sem,
):
    here, feat = lax.axis_index("layer"), lax.axis_index("feat")
    x, zh = here // 2, lax.rem(here, 2)
    zl, core = lax.rem(feat // 2, 2), lax.rem(feat, 2)
    right = (lax.rem(here + 2, 8), feat)
    left = (lax.rem(here + 6, 8), feat)
    across = (here + 1 - 2 * zh, feat)
    twin = (here, feat + 1 - 2 * core)
    near = (here, feat + 2 - 4 * zl)
    ups = tuple((here, lax.rem(feat + 4 * k, 16)) for k in (1, 3, 2))

    def x_feats(d, h):
        return pl.multiple_of(lax.rem(x + d, 4) * 512 + lax.rem(zh + h, 2) * 256, 256)

    def z_feats(h, d):
        return pl.multiple_of(2048 + lax.rem(zh + h, 2) * 1024 + lax.rem(x + d, 4) * 256, 256)

    own = [
        pltpu.make_async_copy(src, re.at[m, pl.ds(0, HALF), :], own_sem.at[m])
        for m, src in enumerate((resid, errors))
    ]
    for c in own:
        c.start()
    loads = {}
    for h in (1, 0):
        for d in range(4):
            for m, w in enumerate((enc, dec)):
                loads["z", m, h, d] = pltpu.make_async_copy(
                    w.at[:, pl.ds(z_feats(h, d), WIDE)], zw.at[m, h, d], w_sem.at[m, 8 + h * 4 + d]
                )
    for s, (d, h) in enumerate(SLOTS):
        for m, w in enumerate((enc, dec)):
            loads["x", m, s] = pltpu.make_async_copy(
                w.at[:, pl.ds(x_feats(d, h), WIDE)], xw.at[m, s], w_sem.at[m, s]
            )
    order = (
        [("z", m, 1, d) for d in range(4) for m in range(2)]
        + [("x", m, s) for s in range(8) for m in range(2)]
        + [("z", m, 0, d) for d in range(4) for m in range(2)]
    )
    for key in order:
        loads[key].start()
    biases = [
        pltpu.make_async_copy(bias.at[pl.ds(x_feats(0, 0), WIDE)], xb, bias_sem.at[0]),
        pltpu.make_async_copy(bias.at[pl.ds(z_feats(0, 0), WIDE)], zb, bias_sem.at[1]),
    ]
    for c in biases:
        c.start()

    barrier = pltpu.get_barrier_semaphore()
    friends = (right, left, across, twin, near) + ups
    for friend in friends:
        pl.semaphore_signal(barrier, inc=1, device_id=friend, device_id_type=MESH)
    pl.semaphore_wait(barrier, len(friends))

    def block(c, half):
        return re.at[:, pl.ds(pl.multiple_of(c * ROWS + half * HALF, HALF), HALF), :]

    def re_copy(src, dst, k, target):
        return pltpu.make_async_remote_copy(
            src_ref=block(*src), dst_ref=block(*dst), send_sem=re_send.at[k],
            recv_sem=re_recv.at[dst[0], dst[1]], device_id=target, device_id_type=MESH,
        )

    first = [re_copy((0, 0), (0, 1), 0, twin), re_copy((0, 0), (1, 0), 1, near)]
    first += [re_copy((0, 0), (2 + i, 0), 2 + i, ups[i]) for i in range(3)]
    second = [re_copy((1, 0), (5 + i, 0), 5 + i, ups[i]) for i in range(3)]

    def forward(c):
        return re_copy((c, 0), (c, 1), 7 + c, twin)

    def arrived(c, half):
        re_copy((c, half), (c, half), 0, twin).wait_recv()

    for c in own:
        c.wait()
    for c in first:
        c.start()

    def copy(kind, c):
        k = KINDS.index(kind)
        src, dst, target = {
            "x1r": (xp.at[c, pl.ds(0, 2)], xr1.at[c, 0], right),
            "x1l": (xp.at[c, pl.ds(2, 2)], xr1.at[c, 1], left),
            "x2r": (xp.at[c, 4], xr2.at[c, 0], right),
            "x2l": (xp.at[c, 5], xr2.at[c, 1], left),
            "xz": (xp.at[c, 7], xzr.at[c], across),
            "xgz": (xo.at[c, 0, 0], xo.at[c, 0, 1], across),
            "xgr0": (xo.at[c, 0, 0], xo.at[c, 3, 0], right),
            "xgl0": (xo.at[c, 0, 0], xo.at[c, 1, 0], left),
            "xgr1": (xo.at[c, 0, 1], xo.at[c, 3, 1], right),
            "xgl1": (xo.at[c, 0, 1], xo.at[c, 1, 1], left),
            "xfr": (xo.at[c, 3, 0], xo.at[c, 2, 0], right),
            "xfl": (xo.at[c, 1, 1], xo.at[c, 2, 1], left),
            "z1": (zp.at[c, 1], zr1.at[c], across),
            "z1r": (zp.at[c, 0, pl.ds(0, 2)], yr1.at[c, 0], right),
            "z1l": (zp.at[c, 0, pl.ds(2, 2)], yr1.at[c, 1], left),
            "z2r": (zp.at[c, 0, 4], yr2.at[c, 0], right),
            "z2l": (zp.at[c, 0, 5], yr2.at[c, 1], left),
            "zgr": (zo.at[c, 0, 0], zo.at[c, 0, 3], right),
            "zgl": (zo.at[c, 0, 0], zo.at[c, 0, 1], left),
            "zfr": (zo.at[c, 0, 3, 0], zo.at[c, 0, 2, 0], right),
            "zfl": (zo.at[c, 0, 1, 1], zo.at[c, 0, 2, 1], left),
            "zz0": (zo.at[c, 0, 0], zo.at[c, 1, 0], across),
            "zz1": (zo.at[c, 0, 1], zo.at[c, 1, 1], across),
            "zz3": (zo.at[c, 0, 3], zo.at[c, 1, 3], across),
            "zz2": (zo.at[c, 0, 2], zo.at[c, 1, 2], across),
        }[kind]
        return pltpu.make_async_remote_copy(
            src_ref=src, dst_ref=dst, send_sem=send_sem.at[k], recv_sem=recv_sem.at[k, c],
            device_id=target, device_id_type=MESH,
        )

    def start(kind, c):
        @pl.when(c > 0)
        def _():
            copy(kind, c - 1).wait_send()

        copy(kind, c).start()

    def got(kind, c):
        copy(kind, c).wait_recv()

    def dot(m, rows, w):
        return jnp.dot(rows[m], w[...], preferred_element_type=F32).astype(BF16)

    def stage0(c):
        @pl.when(c == 0)
        def _():
            arrived(0, 1)
            arrived(1, 0)
            for cc in second:
                cc.start()

        @pl.when(c > 0)
        def _():
            arrived(c, 1)

            @pl.when(c < CHUNKS - 1)
            def _():
                arrived(c + 1, 0)

        @pl.when(c < CHUNKS - 1)
        def _():
            forward(c + 1).start()

        at = pl.ds(pl.multiple_of(c * ROWS, ROWS), ROWS)
        rows = (re[0, at, :], re[1, at, :])

        def ready(*key):
            @pl.when(c == 0)
            def _():
                loads[key].wait()

        def z_part(h):
            for d in range(4):
                for m in range(2):
                    ready("z", m, h, d)
                    got_ = dot(m, rows, zw.at[m, h, d])
                    for half in range(2):
                        zp[c, h, SLOTS.index((d, half)), m] = got_[:, half * NARROW:(half + 1) * NARROW]

        def x_part(slots):
            for s in slots:
                for m in range(2):
                    ready("x", m, s)
                    xp[c, s, m] = dot(m, rows, xw.at[m, s])

        z_part(1)
        start("z1", c)
        x_part((0, 1))
        start("x1r", c)
        x_part((2, 3))
        start("x1l", c)
        x_part((4, 5, 6, 7))
        z_part(0)

    def add(*parts):
        total = parts[0].astype(F32)
        for p in parts[1:]:
            total += p.astype(F32)
        return total

    def stage1(c):
        got("x1r", c)
        xp[c, 4] = add(xp[c, 4], xr1[c, 0, 0]).astype(BF16)
        start("x2r", c)
        got("x1l", c)
        xp[c, 5] = add(xp[c, 5], xr1[c, 1, 0]).astype(BF16)
        start("x2l", c)
        got("z1", c)
        for s in (0, 1):
            zp[c, 0, s] = add(zp[c, 0, s], zr1[c, s]).astype(BF16)
        start("z1r", c)
        for s in (2, 3):
            zp[c, 0, s] = add(zp[c, 0, s], zr1[c, s]).astype(BF16)
        start("z1l", c)

    def stage2(c):
        got("x2l", c)
        xp[c, 7] = add(xp[c, 7], xr2[c, 1], xr1[c, 0, 1]).astype(BF16)
        start("xz", c)
        got("z1r", c)
        zp[c, 0, 4] = add(zp[c, 0, 4], zr1[c, 4], yr1[c, 0, 0]).astype(BF16)
        start("z2r", c)
        got("z1l", c)
        zp[c, 0, 5] = add(zp[c, 0, 5], zr1[c, 5], yr1[c, 1, 0]).astype(BF16)
        start("z2l", c)

    def gate(total, b):
        pre = 4.0 * (total[0] + b[None, :])
        e = jnp.exp(-jnp.abs(pre))
        code = (jnp.maximum(pre, 0.0) + jnp.log1p(e)) * 0.25
        masked = total[1] * (jnp.where(pre >= 0, 1.0, e) / (1.0 + e))
        return masked.astype(BF16), code.astype(BF16)

    def stage3(c):
        got("x2r", c)
        got("xz", c)
        masked, code = gate(add(xp[c, 6], xr2[c, 0], xr1[c, 1, 1], xzr[c]), xb[...])
        xo[c, 0, 0, 0] = masked
        xo[c, 0, 0, 1] = code
        start("xgz", c)
        start("xgr0", c)
        start("xgl0", c)
        got("z2r", c)
        got("z2l", c)
        for half in range(2):
            total = add(zp[c, 0, 6 + half], zr1[c, 6 + half], yr2[c, half], yr1[c, 1 - half, 1])
            masked, code = gate(total, zb[pl.ds(half * NARROW, NARROW)])
            zo[c, 0, 0, half, 0] = masked
            zo[c, 0, 0, half, 1] = code
        start("zgr", c)
        start("zgl", c)
        start("zz0", c)

    def stage4(c):
        got("xgz", c)
        start("xgr1", c)
        start("xgl1", c)
        got("xgr0", c)
        start("xfr", c)
        got("zgr", c)
        start("zfr", c)
        start("zz3", c)
        got("zgl", c)
        start("zfl", c)
        start("zz1", c)

    def stage5(c):
        got("xgl1", c)
        start("xfl", c)
        got("zfr", c)
        got("zfl", c)
        start("zz2", c)

    def stores(c):
        at = pl.ds(pl.multiple_of(c * ROWS, ROWS), ROWS)
        found = []
        for m, out in enumerate((out_masked, out_code)):
            for d in range(4):
                for h in range(2):
                    found.append((xo.at[c, d, h, m], out.at[at, pl.ds(x_feats(d, h), WIDE)]))
                    for half in range(2):
                        found.append((
                            zo.at[c, h, d, half, m],
                            out.at[at, pl.ds(pl.multiple_of(z_feats(h, d) + half * NARROW, NARROW), NARROW)],
                        ))
        return [pltpu.make_async_copy(a, b, out_sem.at[i]) for i, (a, b) in enumerate(found)]

    def stage6(c):
        for kind in ("xgl0", "xgr1", "xfr", "xfl", "zz0", "zz1", "zz3", "zz2"):
            got(kind, c)

        @pl.when(c > 0)
        def _():
            for cc in stores(c - 1):
                cc.wait()

        for cc in stores(c):
            cc.start()

    for c in biases:
        c.wait()

    def step(i, carry):
        for lag, stage in enumerate((stage0, stage1, stage2, stage3, stage4, stage5, stage6)):
            @pl.when((i >= lag) & (i < lag + CHUNKS))
            def _():
                stage(i - lag)

        return carry

    lax.fori_loop(0, CHUNKS + 6, step, 0)

    rout = [
        pltpu.make_async_copy(re.at[m], out, rout_sem.at[m]) for m, out in enumerate((out_resid, out_errors))
    ]
    for c in rout:
        c.start()
    for kind in KINDS:
        copy(kind, CHUNKS - 1).wait_send()
    for c in first + second + [forward(k) for k in range(1, CHUNKS)]:
        c.wait_send()
    for c in rout + stores(CHUNKS - 1):
        c.wait()


def gathered(residuals, errors, enc_weight, dec_weight, enc_bias):
    feats = enc_weight.shape[1]
    tokens = CHUNKS * ROWS
    dma, any_ = pltpu.SemaphoreType.DMA, pl.BlockSpec(memory_space=pl.ANY)
    return pl.pallas_call(
        comm_kernel,
        out_shape=[
            jax.ShapeDtypeStruct((tokens, STACKED), BF16),
            jax.ShapeDtypeStruct((tokens, STACKED), BF16),
            jax.ShapeDtypeStruct((tokens, feats), BF16),
            jax.ShapeDtypeStruct((tokens, feats), BF16),
        ],
        in_specs=[any_] * 5,
        out_specs=[any_] * 4,
        scratch_shapes=[
            pltpu.VMEM((2, tokens, STACKED), BF16),
            pltpu.VMEM((2, 8, STACKED, WIDE), BF16),
            pltpu.VMEM((2, 2, 4, STACKED, WIDE), BF16),
            pltpu.VMEM((WIDE,), F32),
            pltpu.VMEM((WIDE,), F32),
            pltpu.VMEM((CHUNKS, 8, 2, ROWS, WIDE), BF16),
            pltpu.VMEM((CHUNKS, 2, 2, 2, ROWS, WIDE), BF16),
            pltpu.VMEM((CHUNKS, 2, 2, ROWS, WIDE), BF16),
            pltpu.VMEM((CHUNKS, 2, ROWS, WIDE), BF16),
            pltpu.VMEM((CHUNKS, 4, 2, 2, ROWS, WIDE), BF16),
            pltpu.VMEM((CHUNKS, 2, 8, 2, ROWS, NARROW), BF16),
            pltpu.VMEM((CHUNKS, 8, 2, ROWS, NARROW), BF16),
            pltpu.VMEM((CHUNKS, 2, 2, 2, ROWS, NARROW), BF16),
            pltpu.VMEM((CHUNKS, 2, 2, ROWS, NARROW), BF16),
            pltpu.VMEM((CHUNKS, 2, 4, 2, 2, ROWS, NARROW), BF16),
            dma((len(KINDS),)),
            dma((len(KINDS), CHUNKS)),
            dma((15,)),
            dma((CHUNKS, 2)),
            dma((2,)),
            dma((2, 16)),
            dma((48,)),
            dma((2,)),
            dma((2,)),
        ],
        compiler_params=pltpu.CompilerParams(
            collective_id=0, has_side_effects=True, vmem_limit_bytes=60 * 2**20
        ),
    )(residuals, errors, enc_weight, dec_weight, enc_bias)


def transposed(left, right):
    return lax.dot_general(left, right, (((0,), (0,)), ((), ())), preferred_element_type=F32)


def per_device(residuals, errors, enc_weight, dec_weight, enc_bias):
    all_resid, all_errors, masked, code = gathered(residuals, errors, enc_weight, dec_weight, enc_bias)
    enc_grad = transposed(all_resid, masked)
    dec_grad = transposed(all_errors, code)
    bias_grad = jnp.sum(masked.astype(F32), axis=0)
    return enc_grad.astype(BF16), dec_grad.astype(BF16), bias_grad


def solution(mesh):
    placed = (P("feat", "layer"), P("feat", "layer"), P("layer", "feat"), P("layer", "feat"), P("feat"))
    return jax.shard_map(
        per_device,
        mesh=mesh,
        in_specs=placed,
        out_specs=(P("layer", "feat"), P("layer", "feat"), P("feat")),
        check_vma=False,
    )
```
